32 devices in a mesh: section: 4 (over y, core), rep: 2 (over x), tp: 4 (over z).
Axes of the slice: x: 2, y: 2, z: 4, core: 2. Of those that a mesh axis runs over, the one named last changes fastest.
Arguments:
- token_ids: int32 [2, 8, 128], P('rep', None, 'tp'), may hold values from 0 to 16383
- embed: bfloat16 [16384, 1024], P('section'), may hold values from -6 to 6
- w_in: bfloat16 [2, 4, 2, 1024, 2816], P('rep', 'section', None, None, 'tp'), may hold values from -0.1875 to 0.1875
- w_down: bfloat16 [2, 4, 2816, 1024], P('rep', 'section', 'tp'), may hold values from -0.109375 to 0.109375
- outer_in: float32 [4, 2, 1024, 2816], P('section', None, None, 'tp'), may hold values from -0.1875 to 0.1875
- outer_down: float32 [4, 2816, 1024], P('section', 'tp'), may hold values from -0.109375 to 0.109375
- moment_in: float32 [4, 2, 1024, 2816], P('section', None, None, 'tp'), may hold values from -0.12 to 0.12
- moment_down: float32 [4, 2816, 1024], P('section', 'tp'), may hold values from -0.12 to 0.12
- cotangent: bfloat16 [2, 8, 128, 1024], P('rep', None, 'tp'), may hold values from -6 to 6
- fragment: int32 [4], replicated, may hold values 0 or 1
Outputs:
- new_in: bfloat16 [2, 4, 2, 1024, 2816], P('rep', 'section', None, None, 'tp')
- new_down: bfloat16 [2, 4, 2816, 1024], P('rep', 'section', 'tp')
- next_outer_in: float32 [4, 2, 1024, 2816], P('section', None, None, 'tp')
- next_outer_down: float32 [4, 2816, 1024], P('section', 'tp')
- next_moment_in: float32 [4, 2, 1024, 2816], P('section', None, None, 'tp')
- next_moment_down: float32 [4, 2816, 1024], P('section', 'tp')
The draws below stay inside these ranges and needn't reach their ends.
All inputs are finite; a program needn't handle non-finite values.
Results may differ from the reference program's by a relative error of at most 0.03.
Values may be sent and summed in bfloat16 or wider, within the bound.
A program may use at most 128 MiB of HBM per device.

```python
import math
import jax
import jax.numpy as jnp
import numpy as np
from jax import lax

D = 1024
FF = 2816
VOCAB = 16384
MB = 8
MTOK = 128
LAYERS_SECTION = 1
LAYERS = 4
REPS = 2
N_SECTION = 4


def place_ends(drawn, own_key, low, high):
    dims = drawn.shape
    index_at = [jax.random.randint(jax.random.fold_in(own_key, axis), (), 0, dims[axis]) for axis in range(len(dims))]
    drawn = drawn.at[tuple(index_at)].set(low)
    longest = dims.index(max(dims))
    index_at[longest] = (index_at[longest] + 1) % dims[longest]
    return drawn.at[tuple(index_at)].set(high)


def steps_of(key, shape, shards, smallest, top_value):
    def one(dim, shards_of):
        draws = jax.random.uniform(jax.random.fold_in(jax.random.fold_in(key, 6), dim), (shards_of,), jnp.float32, smallest / len(shards), top_value / len(shards))
        return jnp.repeat(jnp.exp(draws), shape[dim] // shards_of).reshape((-1,) + (1,) * (len(shape) - dim - 1))

    loudness = one(*shards[0])
    for cut in shards[1:]:
        loudness = loudness * one(*cut)
    return loudness


def rank_bounds(number_of, slope):
    loads = [(1 << 20) // math.isqrt(rank ** slope) + 1 for rank in range(1, number_of + 1)]
    scale = 1 + sum(loads) // (1 << 30)
    return np.cumsum(np.array([max(1, weight // scale) for weight in loads]))


def ranked(rng, extent, count, slope):
    listing = rank_bounds(count, slope)
    ticket = jax.random.randint(jax.random.fold_in(rng, 1), extent, 0, int(listing[count - 1]))
    grade = jnp.searchsorted(jnp.asarray(listing, jnp.int32), ticket, side="right")
    return jax.random.permutation(jax.random.fold_in(rng, 2), count)[grade].astype(jnp.int32)


def noise(key, dims, scale, most, shards=(), kind=jnp.bfloat16):
    values = scale * jax.random.normal(key, dims, jnp.float32)
    if shards:
        values = values * steps_of(key, dims, shards, -0.22, 0.18)
    return jnp.clip(values, -most, most).astype(kind)


def setup_inputs(seed: int = 0) -> dict:
    arg_keys = jax.random.split(jax.random.key(seed), 11)
    return {
        "token_ids": place_ends(ranked(arg_keys[0], (REPS, MB, MTOK), VOCAB, 2), jax.random.fold_in(arg_keys[0], 3), 0, VOCAB - 1).astype(jnp.int32),
        "embed": noise(arg_keys[1], (VOCAB, D), 1.0, 6.0, ((0, 4),)),
        "w_in": noise(arg_keys[2], (REPS, LAYERS, 2, D, FF), D ** -0.5, 0.1875, ((0, 2), (1, 4), (4, 4))),
        "w_down": noise(arg_keys[3], (REPS, LAYERS, FF, D), FF ** -0.5, 0.109375, ((0, 2), (1, 4), (2, 4))),
        "outer_in": noise(arg_keys[4], (LAYERS, 2, D, FF), D ** -0.5, 0.1875, ((0, 4), (3, 4)), jnp.float32),
        "outer_down": noise(arg_keys[5], (LAYERS, FF, D), FF ** -0.5, 0.109375, ((0, 4), (1, 4)), jnp.float32),
        "moment_in": noise(arg_keys[6], (LAYERS, 2, D, FF), 0.02, 0.12, ((0, 4), (3, 4)), jnp.float32),
        "moment_down": noise(arg_keys[7], (LAYERS, FF, D), 0.02, 0.12, ((0, 4), (1, 4)), jnp.float32),
        "cotangent": noise(arg_keys[8], (REPS, MB, MTOK, D), 1.0, 6.0, ((0, 2), (2, 4))),
        "fragment": place_ends((jax.random.randint(arg_keys[9], (N_SECTION,), 0, 2) < 1).astype(jnp.int32), jax.random.fold_in(arg_keys[9], 1), 0, 1),
    }


EPS = 1e-05
INNER_LR = 0.001
OUTER_LR = 0.7
MOMENTUM = 0.9

def scale_rows(values):
    return lax.rsqrt(lax.optimization_barrier(jnp.mean(values * values, axis=-1, keepdims=True)) + EPS)

def layer_forward(x, pair, down):
    xf = x.astype(jnp.float32)
    rinv = scale_rows(xf)
    normed = (xf * rinv).astype(jnp.bfloat16)
    gate = jnp.dot(normed, pair[0], preferred_element_type=jnp.float32)
    upper = jnp.dot(normed, pair[1], preferred_element_type=jnp.float32)
    hidden = (jax.nn.silu(gate) * upper).astype(jnp.bfloat16)
    out = jnp.dot(hidden, down, preferred_element_type=jnp.float32)
    return ((xf + out).astype(jnp.bfloat16), (normed, gate, upper, hidden))

def layer_backward(grad, x, pair, down, saved):
    normed, gate, upper, hidden = saved
    d_hidden = jnp.dot(grad, down.T, preferred_element_type=jnp.float32)
    sig = jax.nn.sigmoid(gate)
    d_gate = (d_hidden * upper * sig * (1.0 + gate * (1.0 - sig))).astype(jnp.bfloat16)
    d_upper = (d_hidden * jax.nn.silu(gate)).astype(jnp.bfloat16)
    g_down = jnp.dot(hidden.T, grad, preferred_element_type=jnp.float32)
    g_pair = jnp.stack([jnp.dot(normed.T, d_gate, preferred_element_type=jnp.float32), jnp.dot(normed.T, d_upper, preferred_element_type=jnp.float32)])
    d_norm = jnp.dot(d_gate, pair[0].T, preferred_element_type=jnp.float32) + jnp.dot(d_upper, pair[1].T, preferred_element_type=jnp.float32)
    xf = x.astype(jnp.float32)
    rinv = scale_rows(xf)
    d_x = grad.astype(jnp.float32) + rinv * d_norm - xf * (rinv * rinv * rinv) * lax.optimization_barrier(jnp.mean(d_norm * xf, axis=-1, keepdims=True))
    return (d_x.astype(jnp.bfloat16), g_pair, g_down)

def reference(token_ids, embed, w_in, w_down, outer_in, outer_down, moment_in, moment_down, cotangent, fragment):
    chosen = fragment[jnp.arange(LAYERS) // LAYERS_SECTION] == 1
    inner_in = []
    inner_down = []
    for replica in range(REPS):
        x = jnp.take(embed, token_ids[replica].reshape(-1), axis=0)
        inputs = []
        saves = []
        for layer in range(LAYERS):
            inputs.append(x)
            x, saved = layer_forward(x, w_in[replica, layer], w_down[replica, layer])
            saves.append(saved)
        grad = cotangent[replica].reshape(-1, D)
        pair_list = [None] * LAYERS
        down_list = [None] * LAYERS
        for layer in reversed(range(LAYERS)):
            grad, g_pair, g_down = layer_backward(grad, inputs[layer], w_in[replica, layer], w_down[replica, layer], saves[layer])
            pair_list[layer] = (w_in[replica, layer].astype(jnp.float32) - INNER_LR * g_pair).astype(jnp.bfloat16)
            down_list[layer] = (w_down[replica, layer].astype(jnp.float32) - INNER_LR * g_down).astype(jnp.bfloat16)
        inner_in.append(jnp.stack(pair_list))
        inner_down.append(jnp.stack(down_list))
    inner_in = jnp.stack(inner_in)
    inner_down = jnp.stack(inner_down)
    mean_in = lax.optimization_barrier(jnp.mean(outer_in[None] - inner_in.astype(jnp.float32), axis=0))
    mean_down = lax.optimization_barrier(jnp.mean(outer_down[None] - inner_down.astype(jnp.float32), axis=0))
    moment_next_in = MOMENTUM * moment_in + mean_in
    moment_next_down = MOMENTUM * moment_down + mean_down
    outer_next_in = outer_in - OUTER_LR * (mean_in + MOMENTUM * moment_next_in)
    outer_next_down = outer_down - OUTER_LR * (mean_down + MOMENTUM * moment_next_down)
    pick_in = chosen[:, None, None, None]
    pick_down = chosen[:, None, None]
    new_in = jnp.where(pick_in[None], outer_next_in.astype(jnp.bfloat16)[None], inner_in)
    new_down = jnp.where(pick_down[None], outer_next_down.astype(jnp.bfloat16)[None], inner_down)
    return (new_in, new_down, jnp.where(pick_in, outer_next_in, outer_in), jnp.where(pick_down, outer_next_down, outer_down), jnp.where(pick_in, moment_next_in, moment_in), jnp.where(pick_down, moment_next_down, moment_down))
```

```python
import functools

import jax
import jax.numpy as jnp
from jax import lax
from jax.experimental import pallas as pl
from jax.experimental.pallas import tpu as pltpu
from jax.sharding import PartitionSpec as P

EPS = 1e-05
INNER_LR = 0.001
OUTER_LR = 0.7
MOMENTUM = 0.9
STAGE = 5
OWNERS = 2
PIECES = 2
FEEDS = 2
MESH = pl.DeviceIdType.MESH
NT = (((1,), (1,)), ((), ()))


def scale_rows(values):
    return lax.rsqrt(jnp.mean(values * values, axis=-1, keepdims=True) + EPS)


def dot(left, right):
    return jnp.dot(left, right, preferred_element_type=jnp.float32)


def dot_nt(left, right):
    return lax.dot_general(left, right, NT, preferred_element_type=jnp.float32)


def relay(
    sections,
    peers,
    looked,
    seeds,
    pair,
    down,
    normed_out,
    hidden_out,
    d_gate_out,
    d_up_out,
    grad_out,
    x_full,
    grad_full,
    part,
    box,
    mate,
    rows_out,
    back_part,
    back_box,
    back_mate,
    back_rows_out,
    gate_store,
    up_store,
    rows_in,
    looked_box,
    x_recv,
    grad_recv,
    box_recv,
    mate_recv,
    back_box_recv,
    back_mate_recv,
    looked_recv,
    part_send,
    rows_send,
    back_part_send,
    back_rows_send,
    x_first,
    grad_first,
    looked_send,
):
    section = lax.axis_index("section")
    me = lax.axis_index("tp")
    batches, own, _ = looked.shape
    chunks, rows, _ = x_full.shape
    owners = rows // own
    groups = peers // owners
    half = peers // 2
    piece = rows // PIECES
    first = section == 0
    final = section == sections - 1
    later = section < sections - 1
    after = section > 0
    left = me < half
    base = jnp.where(left, 0, half)
    depth = jnp.where(left, me, peers - 1 - me)
    middle = depth == half - 1
    inward = jnp.where(left, me + 1, me - 1)
    my_group = me // owners
    my_rows = pl.ds(pl.multiple_of(lax.rem(me, owners) * own, own), own)

    def wait(ref, sem):
        pltpu.make_async_copy(ref, ref, sem).wait()

    def send(source, target, send_sem, recv_sem, device):
        pltpu.make_async_remote_copy(
            src_ref=source,
            dst_ref=target,
            send_sem=send_sem,
            recv_sem=recv_sem,
            device_id=device,
            device_id_type=MESH,
        ).start()

    def around(offset):
        return lax.rem(me + offset, peers)

    barrier = pltpu.get_barrier_semaphore()
    for offset in range(1, peers):
        pl.semaphore_signal(
            barrier, inc=1, device_id={"tp": around(offset)}, device_id_type=MESH
        )

    @pl.when(later)
    def _():
        for offset in range(peers):
            pl.semaphore_signal(
                barrier,
                inc=1,
                device_id={"section": section + 1, "tp": around(offset)},
                device_id_type=MESH,
            )

    @pl.when(after)
    def _():
        for offset in range(peers):
            pl.semaphore_signal(
                barrier,
                inc=1,
                device_id={"section": section - 1, "tp": around(offset)},
                device_id_type=MESH,
            )

    @pl.when(first)
    def _():
        for other in range(2, sections):
            pl.semaphore_signal(
                barrier, inc=1, device_id={"section": other}, device_id_type=MESH
            )
        pl.semaphore_wait(barrier, 2 * peers - 1 + max(sections - 2, 0))

    @pl.when(section == 1)
    def _():
        pl.semaphore_wait(barrier, (3 if sections > 2 else 2) * peers - 1)

    @pl.when(section >= 2)
    def _():
        pl.semaphore_signal(barrier, inc=1, device_id={"section": 0}, device_id_type=MESH)

    @pl.when((section >= 2) & later)
    def _():
        pl.semaphore_wait(barrier, 3 * peers)

    @pl.when((section >= 2) & final)
    def _():
        pl.semaphore_wait(barrier, 2 * peers)

    def spread(micro, source, full, send_sem, recv_sem):
        chunk = micro * groups + my_group
        for offset in range(1, peers):
            send(
                source.at[micro],
                full.at[chunk, my_rows],
                send_sem.at[micro],
                recv_sem.at[chunk],
                {"tp": around(offset)},
            )
        full[chunk, my_rows, :] = source[micro]

    def feed(micro):
        total = looked[micro]
        for slot in range(sections - 1):
            wait(looked_box.at[slot, micro], looked_recv.at[slot, micro])
            total += looked_box[slot, micro]
        rows_in[micro] = total
        spread(micro, rows_in, x_full, x_first, x_recv)

    @pl.when(after)
    def _():
        def give(micro, carry):
            send(
                looked.at[micro],
                looked_box.at[section - 1, micro],
                looked_send.at[micro],
                looked_recv.at[section - 1, micro],
                {"section": 0},
            )
            return carry

        lax.fori_loop(0, batches, give, 0)

    @pl.when(final)
    def _():
        def give(micro, carry):
            spread(micro, seeds, grad_full, grad_first, grad_recv)
            return carry

        lax.fori_loop(0, batches, give, 0)

    @pl.when(first)
    def _():
        for micro in range(min(FEEDS, batches)):
            feed(micro)

    def arrive(chunk, full, recv_sem, source):
        mine = source & (lax.rem(chunk, groups) == my_group)

        @pl.when(jnp.logical_not(mine))
        def _():
            wait(full.at[chunk], recv_sem.at[chunk])

        if owners > 1:

            @pl.when(mine)
            def _():
                wait(full.at[chunk, pl.ds(0, rows - own)], recv_sem.at[chunk])

    def push(chunk, index, source, box, mate, send_sem, box_sem, mate_sem):
        span = pl.ds(index * piece, piece)

        @pl.when(middle)
        def _():
            send(
                source.at[chunk, span],
                mate.at[chunk, span],
                send_sem.at[chunk],
                mate_sem.at[chunk, index],
                {"tp": peers - 1 - me},
            )

        @pl.when(jnp.logical_not(middle))
        def _():
            send(
                source.at[chunk, span],
                box.at[chunk, span],
                send_sem.at[chunk],
                box_sem.at[chunk, index],
                {"tp": inward},
            )

    def join(chunk, source, box, mate, send_sem, box_sem, mate_sem):
        for index in range(PIECES):
            span = pl.ds(index * piece, piece)
            wait(box.at[chunk, span], box_sem.at[chunk, index])
            total = source[chunk, span, :].astype(jnp.float32)
            total += box[chunk, span, :].astype(jnp.float32)
            source[chunk, span, :] = total.astype(jnp.bfloat16)
            push(chunk, index, source, box, mate, send_sem, box_sem, mate_sem)

    def pass_along(chunk, span, source, full, send_sem, recv_sem, step):
        for offset in range(half):
            send(
                source.at[chunk, span],
                full.at[chunk, span],
                send_sem.at[chunk],
                recv_sem.at[chunk],
                {"section": section + step, "tp": base + offset},
            )

    forward_way = (part, box, mate, part_send, box_recv, mate_recv)
    backward_way = (
        back_part,
        back_box,
        back_mate,
        back_part_send,
        back_box_recv,
        back_mate_recv,
    )

    def forward(chunk):
        arrive(chunk, x_full, x_recv, first)
        xf = x_full[chunk].astype(jnp.float32)
        normed = (xf * scale_rows(xf)).astype(jnp.bfloat16)
        normed_out[chunk] = normed
        gate = dot(normed, pair[0])
        upper = dot(normed, pair[1])
        gate_store[chunk] = gate
        up_store[chunk] = upper
        hidden = (gate * jax.nn.sigmoid(gate) * upper).astype(jnp.bfloat16)
        hidden_out[chunk] = hidden

        @pl.when(later)
        def _():
            part[chunk] = dot(hidden, down[...]).astype(jnp.bfloat16)

            @pl.when(depth == 0)
            def _():
                for index in range(PIECES):
                    push(chunk, index, *forward_way)

    def forward_join(chunk):
        join(chunk, *forward_way)

    def forward_end(chunk):
        for index in range(PIECES):
            span = pl.ds(index * piece, piece)
            wait(mate.at[chunk, span], mate_recv.at[chunk, index])
            total = part[chunk, span, :].astype(jnp.float32)
            total += mate[chunk, span, :].astype(jnp.float32)
            xf = x_full[chunk, span, :].astype(jnp.float32)
            rows_out[chunk, span, :] = (xf + total).astype(jnp.bfloat16)
            pass_along(chunk, span, rows_out, x_full, rows_send, x_recv, 1)

    def backward(chunk):
        arrive(chunk, grad_full, grad_recv, final)
        grad = grad_full[chunk]
        grad_out[chunk] = grad
        d_hidden = dot_nt(grad, down[...])
        gate = gate_store[chunk]
        sig = jax.nn.sigmoid(gate)
        d_gate = (d_hidden * up_store[chunk] * sig * (1.0 + gate * (1.0 - sig))).astype(
            jnp.bfloat16
        )
        d_up = (d_hidden * (gate * sig)).astype(jnp.bfloat16)
        d_gate_out[chunk] = d_gate
        d_up_out[chunk] = d_up

        @pl.when(after)
        def _():
            back_part[chunk] = (dot_nt(d_gate, pair[0]) + dot_nt(d_up, pair[1])).astype(
                jnp.bfloat16
            )

            @pl.when(depth == 0)
            def _():
                for index in range(PIECES):
                    push(chunk, index, *backward_way)

    def backward_join(chunk):
        join(chunk, *backward_way)

    def backward_end(chunk):
        for index in range(PIECES):
            span = pl.ds(index * piece, piece)
            wait(back_mate.at[chunk, span], back_mate_recv.at[chunk, index])
            d_norm = back_part[chunk, span, :].astype(jnp.float32)
            d_norm += back_mate[chunk, span, :].astype(jnp.float32)
            xf = x_full[chunk, span, :].astype(jnp.float32)
            rinv = scale_rows(xf)
            d_x = (
                grad_full[chunk, span, :].astype(jnp.float32)
                + rinv * d_norm
                - xf * (rinv * rinv * rinv) * jnp.mean(d_norm * xf, axis=-1, keepdims=True)
            )
            back_rows_out[chunk, span, :] = d_x.astype(jnp.bfloat16)
            pass_along(chunk, span, back_rows_out, grad_full, back_rows_send, grad_recv, -1)

    ahead = STAGE * section
    behind = STAGE * (2 * (sections - 1) - section)

    def step(tick, carry):
        def on(condition, offset, task):
            chunk = tick - offset

            @pl.when(condition & (chunk >= 0) & (chunk < chunks))
            def _():
                task(chunk)

        fed = tick // groups + FEEDS

        @pl.when(first & (lax.rem(tick, groups) == 0) & (fed < batches))
        def _():
            feed(fed)

        on(section >= 0, ahead, forward)
        on(later & (depth > 0), ahead, forward_join)
        on(section >= 0, behind, backward)
        on(after & (depth > 0), behind, backward_join)
        on(after & middle, behind + 1, backward_end)
        on(later & middle, ahead + 1, forward_end)
        return carry

    lax.fori_loop(0, chunks + 2 * STAGE * (sections - 1) + 1, step, 0)

    def drain_feeds(micro, carry):
        others = rows_in.at[pl.ds(0, peers - 1)]

        @pl.when(first)
        def _():
            wait(others, x_first.at[micro])

        @pl.when(final)
        def _():
            wait(others, grad_first.at[micro])

        @pl.when(after)
        def _():
            wait(looked.at[micro], looked_send.at[micro])

        return carry

    lax.fori_loop(0, batches, drain_feeds, 0)

    def drain(chunk, carry):
        @pl.when(later)
        def _():
            wait(part.at[chunk], part_send.at[chunk])

        @pl.when(after)
        def _():
            wait(back_part.at[chunk], back_part_send.at[chunk])

        @pl.when(later & middle)
        def _():
            wait(rows_out.at[pl.ds(0, half)], rows_send.at[chunk])

        @pl.when(after & middle)
        def _():
            wait(back_rows_out.at[pl.ds(0, half)], back_rows_send.at[chunk])

        return carry

    lax.fori_loop(0, chunks, drain, 0)


def run_relay(x0, seeds, pair, down):
    sections, peers = lax.axis_size("section"), lax.axis_size("tp")
    batches, own, width = x0.shape
    hidden = down.shape[0]
    owners = min(OWNERS, peers)
    rows = own * owners
    chunks = batches * peers // owners

    def of(columns, kind=jnp.bfloat16):
        return pltpu.VMEM((chunks, rows, columns), kind)

    def out(columns):
        return jax.ShapeDtypeStruct((chunks, rows, columns), jnp.bfloat16)

    def sems(*shape):
        return pltpu.SemaphoreType.DMA(shape)

    vmem = pl.BlockSpec(memory_space=pltpu.VMEM)
    flops = 2 * chunks * rows * width * hidden * 6
    return pl.pallas_call(
        functools.partial(relay, sections, peers),
        out_shape=(out(width), out(hidden), out(hidden), out(hidden), out(width)),
        in_specs=[vmem] * 4,
        out_specs=(vmem,) * 5,
        scratch_shapes=[of(width)] * 10
        + [of(hidden, kind=jnp.float32)] * 2
        + [
            pltpu.VMEM((batches, own, width), jnp.bfloat16),
            pltpu.VMEM((sections - 1, batches, own, width), jnp.bfloat16),
            sems(chunks),
            sems(chunks),
            sems(chunks, PIECES),
            sems(chunks, PIECES),
            sems(chunks, PIECES),
            sems(chunks, PIECES),
            sems(sections - 1, batches),
            sems(chunks),
            sems(chunks),
            sems(chunks),
            sems(chunks),
            sems(batches),
            sems(batches),
            sems(batches),
        ],
        compiler_params=pltpu.CompilerParams(
            collective_id=0, has_side_effects=True, vmem_limit_bytes=60 * 1024 * 1024
        ),
        cost_estimate=pl.CostEstimate(
            flops=flops, bytes_accessed=32 * 1024 * 1024, transcendentals=0
        ),
    )(x0, seeds, pair, down)


def shards(
    token_ids,
    embed,
    w_in,
    w_down,
    outer_in,
    outer_down,
    moment_in,
    moment_down,
    cotangent,
    fragment,
):
    sections = lax.axis_size("section")
    section = lax.axis_index("section")
    replicas = lax.axis_size("rep")
    ids = token_ids[0]
    batches, own_rows = ids.shape
    vocab_part, width = embed.shape
    local_ids = ids - section * vocab_part
    inside = (local_ids >= 0) & (local_ids < vocab_part)
    looked = jnp.take(embed, jnp.clip(local_ids, 0, vocab_part - 1), axis=0)
    start_rows = jnp.where(inside[:, :, None], looked, jnp.zeros_like(looked))
    pairs = w_in[0, 0]
    downs = w_down[0, 0]
    normed, hidden, d_gate, d_up, grad = run_relay(start_rows, cotangent[0], pairs, downs)

    def weight_grad(left, right):
        return jnp.einsum("bti,btj->ij", left, right, preferred_element_type=jnp.float32)

    def other(values):
        return lax.ppermute(
            values, "rep", [(source, (source + 1) % replicas) for source in range(replicas)]
        )

    def total(values):
        summed = values.astype(jnp.float32)
        passing = values
        for _ in range(replicas - 1):
            passing = other(passing)
            summed = summed + passing.astype(jnp.float32)
        return summed

    def inner(weights, grads):
        return (weights.astype(jnp.float32) - INNER_LR * grads).astype(jnp.bfloat16)

    flag = lax.dynamic_index_in_dim(fragment, section, 0, keepdims=False)
    chosen = flag == 1

    new = (
        inner(downs, weight_grad(hidden, grad)),
        inner(pairs[0], weight_grad(normed, d_gate)),
        inner(pairs[1], weight_grad(normed, d_up)),
    )
    outers = (outer_down[0], outer_in[0, 0], outer_in[0, 1])
    moments = (moment_down[0], moment_in[0, 0], moment_in[0, 1])

    def finish(trio):
        down, gate, up = trio
        return jnp.stack([gate, up])[None], down[None]

    def synchronize():
        results = []
        for fresh, outer, moment in zip(new, outers, moments):
            mean = outer - total(fresh) / replicas
            next_moment = MOMENTUM * moment + mean
            next_outer = outer - OUTER_LR * (mean + MOMENTUM * next_moment)
            results.append((next_outer.astype(jnp.bfloat16), next_outer, next_moment))
        return tuple(finish(trio) for trio in zip(*results))

    def keep():
        return finish(new), (outer_in, outer_down), (moment_in, moment_down)

    (news, outer_results, moment_results) = lax.cond(chosen, synchronize, keep)
    return (news[0][None], news[1][None]) + outer_results + moment_results


def solution(mesh):
    return jax.shard_map(
        shards,
        mesh=mesh,
        in_specs=(
            P("rep", None, "tp"),
            P("section", None),
            P("rep", "section", None, None, "tp"),
            P("rep", "section", "tp", None),
            P("section", None, None, "tp"),
            P("section", "tp", None),
            P("section", None, None, "tp"),
            P("section", "tp", None),
            P("rep", None, "tp", None),
            P(),
        ),
        out_specs=(
            P("rep", "section", None, None, "tp"),
            P("rep", "section", "tp", None),
            P("section", None, None, "tp"),
            P("section", "tp", None),
            P("section", None, None, "tp"),
            P("section", "tp", None),
        ),
        check_vma=False,
    )
```

```python
import functools

import jax
import jax.numpy as jnp
from jax import lax
from jax.experimental import pallas as pl
from jax.experimental.pallas import tpu as pltpu
from jax.sharding import PartitionSpec as P

EPS = 1e-05
INNER_LR = 0.001
OUTER_LR = 0.7
MOMENTUM = 0.9
STAGE = 5
OWNERS = 2
PIECES = 2
FEEDS = 2
WEIGHT_ROWS = 256
BLOCK = 176
MESH = pl.DeviceIdType.MESH
NT = (((1,), (1,)), ((), ()))
TN = (((0,), (0,)), ((), ()))


def scale_rows(values):
    return lax.rsqrt(jnp.mean(values * values, axis=-1, keepdims=True) + EPS)


def dot(left, right):
    return jnp.dot(left, right, preferred_element_type=jnp.float32)


def dot_nt(left, right):
    return lax.dot_general(left, right, NT, preferred_element_type=jnp.float32)


def dot_tn(left, right):
    return lax.dot_general(left, right, TN, preferred_element_type=jnp.float32)


def relay(
    sections,
    peers,
    looked,
    seeds,
    pair,
    down,
    new_down,
    new_gate,
    new_up,
    x_full,
    grad_full,
    part,
    box,
    mate,
    rows_out,
    back_part,
    back_box,
    back_mate,
    back_rows_out,
    gate_store,
    up_store,
    normed_out,
    hidden_out,
    d_gate_out,
    d_up_out,
    sum_down,
    sum_gate,
    sum_up,
    rows_in,
    looked_box,
    x_recv,
    grad_recv,
    box_recv,
    mate_recv,
    back_box_recv,
    back_mate_recv,
    looked_recv,
    part_send,
    rows_send,
    back_part_send,
    back_rows_send,
    x_first,
    grad_first,
    looked_send,
):
    section = lax.axis_index("section")
    me = lax.axis_index("tp")
    batches, own, _ = looked.shape
    chunks, rows, _ = x_full.shape
    owners = rows // own
    groups = peers // owners
    half = peers // 2
    piece = rows // PIECES
    first = section == 0
    final = section == sections - 1
    later = section < sections - 1
    after = section > 0
    left = me < half
    base = jnp.where(left, 0, half)
    depth = jnp.where(left, me, peers - 1 - me)
    middle = depth == half - 1
    inward = jnp.where(left, me + 1, me - 1)
    my_group = me // owners
    my_rows = pl.ds(pl.multiple_of(lax.rem(me, owners) * own, own), own)

    def wait(ref, sem):
        pltpu.make_async_copy(ref, ref, sem).wait()

    def send(source, target, send_sem, recv_sem, device):
        pltpu.make_async_remote_copy(
            src_ref=source,
            dst_ref=target,
            send_sem=send_sem,
            recv_sem=recv_sem,
            device_id=device,
            device_id_type=MESH,
        ).start()

    def around(offset):
        return lax.rem(me + offset, peers)

    for total in (sum_down, sum_gate, sum_up):
        total[...] = jnp.zeros_like(total)

    barrier = pltpu.get_barrier_semaphore()
    for offset in range(1, peers):
        pl.semaphore_signal(
            barrier, inc=1, device_id={"tp": around(offset)}, device_id_type=MESH
        )

    @pl.when(later)
    def _():
        for offset in range(peers):
            pl.semaphore_signal(
                barrier,
                inc=1,
                device_id={"section": section + 1, "tp": around(offset)},
                device_id_type=MESH,
            )

    @pl.when(after)
    def _():
        for offset in range(peers):
            pl.semaphore_signal(
                barrier,
                inc=1,
                device_id={"section": section - 1, "tp": around(offset)},
                device_id_type=MESH,
            )

    @pl.when(first)
    def _():
        for other in range(2, sections):
            pl.semaphore_signal(
                barrier, inc=1, device_id={"section": other}, device_id_type=MESH
            )
        pl.semaphore_wait(barrier, 2 * peers - 1 + max(sections - 2, 0))

    @pl.when(section == 1)
    def _():
        pl.semaphore_wait(barrier, (3 if sections > 2 else 2) * peers - 1)

    @pl.when(section >= 2)
    def _():
        pl.semaphore_signal(barrier, inc=1, device_id={"section": 0}, device_id_type=MESH)

    @pl.when((section >= 2) & later)
    def _():
        pl.semaphore_wait(barrier, 3 * peers)

    @pl.when((section >= 2) & final)
    def _():
        pl.semaphore_wait(barrier, 2 * peers)

    def spread(micro, source, full, send_sem, recv_sem):
        chunk = micro * groups + my_group
        for offset in range(1, peers):
            send(
                source.at[micro],
                full.at[chunk, my_rows],
                send_sem.at[micro],
                recv_sem.at[chunk],
                {"tp": around(offset)},
            )
        full[chunk, my_rows, :] = source[micro]

    def feed(micro):
        total = looked[micro]
        for slot in range(sections - 1):
            wait(looked_box.at[slot, micro], looked_recv.at[slot, micro])
            total += looked_box[slot, micro]
        rows_in[micro] = total
        spread(micro, rows_in, x_full, x_first, x_recv)

    @pl.when(after)
    def _():
        def give(micro, carry):
            send(
                looked.at[micro],
                looked_box.at[section - 1, micro],
                looked_send.at[micro],
                looked_recv.at[section - 1, micro],
                {"section": 0},
            )
            return carry

        lax.fori_loop(0, batches, give, 0)

    @pl.when(final)
    def _():
        def give(micro, carry):
            spread(micro, seeds, grad_full, grad_first, grad_recv)
            return carry

        lax.fori_loop(0, batches, give, 0)

    @pl.when(first)
    def _():
        for micro in range(min(FEEDS, batches)):
            feed(micro)

    def arrive(chunk, full, recv_sem, source):
        mine = source & (lax.rem(chunk, groups) == my_group)

        @pl.when(jnp.logical_not(mine))
        def _():
            wait(full.at[chunk], recv_sem.at[chunk])

        if owners > 1:

            @pl.when(mine)
            def _():
                wait(full.at[chunk, pl.ds(0, rows - own)], recv_sem.at[chunk])

    def push(chunk, index, source, box, mate, send_sem, box_sem, mate_sem):
        span = pl.ds(index * piece, piece)

        @pl.when(middle)
        def _():
            send(
                source.at[chunk, span],
                mate.at[chunk, span],
                send_sem.at[chunk],
                mate_sem.at[chunk, index],
                {"tp": peers - 1 - me},
            )

        @pl.when(jnp.logical_not(middle))
        def _():
            send(
                source.at[chunk, span],
                box.at[chunk, span],
                send_sem.at[chunk],
                box_sem.at[chunk, index],
                {"tp": inward},
            )

    def join(chunk, source, box, mate, send_sem, box_sem, mate_sem):
        for index in range(PIECES):
            span = pl.ds(index * piece, piece)
            wait(box.at[chunk, span], box_sem.at[chunk, index])
            total = source[chunk, span, :].astype(jnp.float32)
            total += box[chunk, span, :].astype(jnp.float32)
            source[chunk, span, :] = total.astype(jnp.bfloat16)
            push(chunk, index, source, box, mate, send_sem, box_sem, mate_sem)

    def pass_along(chunk, span, source, full, send_sem, recv_sem, step):
        for offset in range(half):
            send(
                source.at[chunk, span],
                full.at[chunk, span],
                send_sem.at[chunk],
                recv_sem.at[chunk],
                {"section": section + step, "tp": base + offset},
            )

    forward_way = (part, box, mate, part_send, box_recv, mate_recv)
    backward_way = (
        back_part,
        back_box,
        back_mate,
        back_part_send,
        back_box_recv,
        back_mate_recv,
    )

    def forward(chunk):
        arrive(chunk, x_full, x_recv, first)
        xf = x_full[chunk].astype(jnp.float32)
        normed = (xf * scale_rows(xf)).astype(jnp.bfloat16)
        normed_out[chunk] = normed
        gate = dot_nt(normed, pair[0])
        upper = dot_nt(normed, pair[1])
        gate_store[chunk] = gate
        up_store[chunk] = upper
        hidden = (gate * jax.nn.sigmoid(gate) * upper).astype(jnp.bfloat16)
        hidden_out[chunk] = hidden

        @pl.when(later)
        def _():
            part[chunk] = dot(hidden, down[...]).astype(jnp.bfloat16)

            @pl.when(depth == 0)
            def _():
                for index in range(PIECES):
                    push(chunk, index, *forward_way)

    def forward_join(chunk):
        join(chunk, *forward_way)

    def forward_end(chunk):
        for index in range(PIECES):
            span = pl.ds(index * piece, piece)
            wait(mate.at[chunk, span], mate_recv.at[chunk, index])
            total = part[chunk, span, :].astype(jnp.float32)
            total += mate[chunk, span, :].astype(jnp.float32)
            xf = x_full[chunk, span, :].astype(jnp.float32)
            rows_out[chunk, span, :] = (xf + total).astype(jnp.bfloat16)
            pass_along(chunk, span, rows_out, x_full, rows_send, x_recv, 1)

    def backward(chunk):
        arrive(chunk, grad_full, grad_recv, final)
        grad = grad_full[chunk]
        d_hidden = dot_nt(grad, down[...])
        gate = gate_store[chunk]
        sig = jax.nn.sigmoid(gate)
        d_gate = (d_hidden * up_store[chunk] * sig * (1.0 + gate * (1.0 - sig))).astype(
            jnp.bfloat16
        )
        d_up = (d_hidden * (gate * sig)).astype(jnp.bfloat16)
        d_gate_out[chunk] = d_gate
        d_up_out[chunk] = d_up

        @pl.when(after)
        def _():
            back_part[chunk] = (dot(d_gate, pair[0]) + dot(d_up, pair[1])).astype(
                jnp.bfloat16
            )

            @pl.when(depth == 0)
            def _():
                for index in range(PIECES):
                    push(chunk, index, *backward_way)

    def backward_join(chunk):
        join(chunk, *backward_way)

    def backward_end(chunk):
        for index in range(PIECES):
            span = pl.ds(index * piece, piece)
            wait(back_mate.at[chunk, span], back_mate_recv.at[chunk, index])
            d_norm = back_part[chunk, span, :].astype(jnp.float32)
            d_norm += back_mate[chunk, span, :].astype(jnp.float32)
            xf = x_full[chunk, span, :].astype(jnp.float32)
            rinv = scale_rows(xf)
            d_x = (
                grad_full[chunk, span, :].astype(jnp.float32)
                + rinv * d_norm
                - xf * (rinv * rinv * rinv) * jnp.mean(d_norm * xf, axis=-1, keepdims=True)
            )
            back_rows_out[chunk, span, :] = d_x.astype(jnp.bfloat16)
            pass_along(chunk, span, back_rows_out, grad_full, back_rows_send, grad_recv, -1)

    bundle = min(chunks, max(1, WEIGHT_ROWS // rows))
    bundles = chunks // bundle

    def weigh(which, left, right, weights, total, out):
        span = pl.ds(which * bundle, bundle)
        rows_of = bundle * rows
        update = dot_tn(
            left[span].reshape(rows_of, left.shape[2]),
            right[span].reshape(rows_of, right.shape[2]),
        )

        @pl.when(which < bundles - 1)
        def _():
            total[...] += update

        @pl.when(which == bundles - 1)
        def _():
            grads = total[...] + update
            out[...] = (weights.astype(jnp.float32) - INNER_LR * grads).astype(jnp.bfloat16)

    weighings = (
        lambda which: weigh(which, hidden_out, grad_full, down[...], sum_down, new_down),
        lambda which: weigh(which, d_gate_out, normed_out, pair[0], sum_gate, new_gate),
        lambda which: weigh(which, d_up_out, normed_out, pair[1], sum_up, new_up),
    )
    ahead = STAGE * section
    behind = STAGE * (2 * (sections - 1) - section)

    def step(tick, carry):
        def on(condition, offset, task):
            chunk = tick - offset

            @pl.when(condition & (chunk >= 0) & (chunk < chunks))
            def _():
                task(chunk)

        fed = tick // groups + FEEDS

        @pl.when(first & (lax.rem(tick, groups) == 0) & (fed < batches))
        def _():
            feed(fed)

        on(section >= 0, ahead, forward)
        on(later & (depth > 0), ahead, forward_join)
        on(section >= 0, behind, backward)
        on(after & (depth > 0), behind, backward_join)
        on(after & middle, behind + 1, backward_end)
        on(later & middle, ahead + 1, forward_end)
        for turn, weighing in enumerate(weighings):
            since = tick - behind - (bundle - 1) - turn

            @pl.when((since >= 0) & (since < chunks) & (lax.rem(since, bundle) == 0))
            def _():
                weighing(since // bundle)

        return carry

    lax.fori_loop(0, chunks + 2 * STAGE * (sections - 1) + 2, step, 0)

    def drain_feeds(micro, carry):
        others = rows_in.at[pl.ds(0, peers - 1)]

        @pl.when(first)
        def _():
            wait(others, x_first.at[micro])

        @pl.when(final)
        def _():
            wait(others, grad_first.at[micro])

        @pl.when(after)
        def _():
            wait(looked.at[micro], looked_send.at[micro])

        return carry

    lax.fori_loop(0, batches, drain_feeds, 0)

    def drain(chunk, carry):
        @pl.when(later)
        def _():
            wait(part.at[chunk], part_send.at[chunk])

        @pl.when(after)
        def _():
            wait(back_part.at[chunk], back_part_send.at[chunk])

        @pl.when(later & middle)
        def _():
            wait(rows_out.at[pl.ds(0, half)], rows_send.at[chunk])

        @pl.when(after & middle)
        def _():
            wait(back_rows_out.at[pl.ds(0, half)], back_rows_send.at[chunk])

        return carry

    lax.fori_loop(0, chunks, drain, 0)


def run_relay(x0, seeds, pair, down):
    sections, peers = lax.axis_size("section"), lax.axis_size("tp")
    batches, own, width = x0.shape
    hidden = down.shape[0]
    owners = min(OWNERS, peers)
    rows = own * owners
    chunks = batches * peers // owners

    def of(columns, kind=jnp.bfloat16):
        return pltpu.VMEM((chunks, rows, columns), kind)

    def like(kind):
        return pltpu.VMEM((hidden, width), kind)

    def sems(*shape):
        return pltpu.SemaphoreType.DMA(shape)

    vmem = pl.BlockSpec(memory_space=pltpu.VMEM)
    flops = 2 * chunks * rows * width * hidden * 9
    return pl.pallas_call(
        functools.partial(relay, sections, peers),
        out_shape=(jax.ShapeDtypeStruct((hidden, width), jnp.bfloat16),) * 3,
        in_specs=[vmem] * 4,
        out_specs=(vmem,) * 3,
        scratch_shapes=[of(width)] * 10
        + [of(hidden, kind=jnp.float32)] * 2
        + [of(width)]
        + [of(hidden)] * 3
        + [like(jnp.float32)] * 3
        + [
            pltpu.VMEM((batches, own, width), jnp.bfloat16),
            pltpu.VMEM((sections - 1, batches, own, width), jnp.bfloat16),
            sems(chunks),
            sems(chunks),
            sems(chunks, PIECES),
            sems(chunks, PIECES),
            sems(chunks, PIECES),
            sems(chunks, PIECES),
            sems(sections - 1, batches),
            sems(chunks),
            sems(chunks),
            sems(chunks),
            sems(chunks),
            sems(batches),
            sems(batches),
            sems(batches),
        ],
        compiler_params=pltpu.CompilerParams(
            collective_id=0, has_side_effects=True, vmem_limit_bytes=63 * 1024 * 1024
        ),
        cost_estimate=pl.CostEstimate(
            flops=flops, bytes_accessed=32 * 1024 * 1024, transcendentals=0
        ),
    )(x0, seeds, pair, down)


def outer_step(replicas, *refs):
    shared = [ref[...].astype(jnp.float32) for ref in refs[:replicas]]
    outer, moment = refs[replicas][0], refs[replicas + 1][0]
    new, next_outer, next_moment = refs[-3:]
    mean = outer - sum(shared) / replicas
    moved = MOMENTUM * moment + mean
    stepped = outer - OUTER_LR * (mean + MOMENTUM * moved)
    new[0] = stepped.astype(jnp.bfloat16)
    next_outer[0] = stepped
    next_moment[0] = moved


def keep_step(fresh, outer, moment, *refs):
    new, next_outer, next_moment = refs[-3:]
    new[0] = fresh[...]
    next_outer[...] = outer[...]
    next_moment[...] = moment[...]


def step_part(index, shared, outer, moment, earlier):
    replicas = len(shared)
    parts, rows, width = outer.shape
    block = next(size for size in range(min(BLOCK, rows), 0, -1) if rows % size == 0)
    one = pl.BlockSpec((block, width), lambda i: (i, 0))
    part = pl.BlockSpec((1, block, width), lambda i: (index, i, 0))
    anywhere = pl.BlockSpec(memory_space=pl.ANY)
    first = replicas + 2

    return pl.pallas_call(
        keep_step if replicas == 1 else functools.partial(outer_step, replicas),
        grid=(rows // block,),
        out_shape=(
            pltpu.HBM(outer.shape, jnp.bfloat16),
            pltpu.HBM(outer.shape, jnp.float32),
            pltpu.HBM(outer.shape, jnp.float32),
        ),
        in_specs=[one] * replicas + [part] * 2 + [anywhere] * len(earlier),
        out_specs=(part,) * 3,
        input_output_aliases={first + place: place for place in range(len(earlier))},
        compiler_params=pltpu.CompilerParams(vmem_limit_bytes=24 * 1024 * 1024),
        cost_estimate=pl.CostEstimate(
            flops=10 * rows * width, bytes_accessed=24 * rows * width, transcendentals=0
        ),
    )(*shared, outer, moment, *earlier)


def shards(
    token_ids,
    embed,
    w_in,
    w_down,
    outer_in,
    outer_down,
    moment_in,
    moment_down,
    cotangent,
    fragment,
):
    section = lax.axis_index("section")
    replicas = lax.axis_size("rep")
    ids = token_ids[0]
    vocab_part, width = embed.shape
    local_ids = ids - section * vocab_part
    inside = (local_ids >= 0) & (local_ids < vocab_part)
    looked = jnp.take(embed, jnp.clip(local_ids, 0, vocab_part - 1), axis=0)
    start_rows = jnp.where(inside[:, :, None], looked, jnp.zeros_like(looked))

    def turned(values):
        return jnp.swapaxes(values, -1, -2)

    new_down, new_gate, new_up = run_relay(
        start_rows, cotangent[0], turned(w_in[0, 0]), w_down[0, 0]
    )

    def shared(values):
        everyone = [values]
        for _ in range(replicas - 1):
            everyone.append(
                lax.ppermute(
                    everyone[-1],
                    "rep",
                    [(source, (source + 1) % replicas) for source in range(replicas)],
                )
            )
        return everyone

    flag = lax.dynamic_index_in_dim(fragment, section, 0, keepdims=False)

    outer_turned, moment_turned = turned(outer_in[0]), turned(moment_in[0])

    def step(gates, ups, downs):
        ins = step_part(0, gates, outer_turned, moment_turned, ())
        ins = step_part(1, ups, outer_turned, moment_turned, ins)
        down = step_part(0, downs, outer_down, moment_down, ())
        return (ins[0], down[0], ins[1], down[1], ins[2], down[2])

    def synchronize():
        return step(shared(new_gate), shared(new_up), shared(new_down))

    def keep():
        return step([new_gate], [new_up], [new_down])

    new_in, new_down, outer_in, outer_down, moment_in, moment_down = lax.cond(
        flag == 1, synchronize, keep
    )
    return (
        turned(new_in)[None, None],
        new_down[None],
        turned(outer_in)[None],
        outer_down,
        turned(moment_in)[None],
        moment_down,
    )


def solution(mesh):
    return jax.shard_map(
        shards,
        mesh=mesh,
        in_specs=(
            P("rep", None, "tp"),
            P("section", None),
            P("rep", "section", None, None, "tp"),
            P("rep", "section", "tp", None),
            P("section", None, None, "tp"),
            P("section", "tp", None),
            P("section", None, None, "tp"),
            P("section", "tp", None),
            P("rep", None, "tp", None),
            P(),
        ),
        out_specs=(
            P("rep", "section", None, None, "tp"),
            P("rep", "section", "tp", None),
            P("section", None, None, "tp"),
            P("section", "tp", None),
            P("section", None, None, "tp"),
            P("section", "tp", None),
        ),
        check_vma=False,
    )
```

```python
import functools

import jax
import jax.numpy as jnp
from jax import lax
from jax.experimental import pallas as pl
from jax.experimental.pallas import tpu as pltpu
from jax.sharding import PartitionSpec as P

EPS = 1e-05
INNER_LR = 0.001
OUTER_LR = 0.7
MOMENTUM = 0.9
STAGE = 4
OWNERS = 2
PIECES = 2
FEEDS = 4
PASSES = 4
WEIGHT_ROWS = 256
BLOCK = 176
MESH = pl.DeviceIdType.MESH
NT = (((1,), (1,)), ((), ()))
TN = (((0,), (0,)), ((), ()))


def scale_rows(values):
    return lax.rsqrt(jnp.mean(values * values, axis=-1, keepdims=True) + EPS)


def dot(left, right):
    return jnp.dot(left, right, preferred_element_type=jnp.float32)


def dot_nt(left, right):
    return lax.dot_general(left, right, NT, preferred_element_type=jnp.float32)


def dot_tn(left, right):
    return lax.dot_general(left, right, TN, preferred_element_type=jnp.float32)


def relay(
    sections,
    peers,
    vocab_part,
    looked,
    ids,
    seeds,
    pair_here,
    down_here,
    new_down,
    new_up,
    new_gate_top,
    new_gate_rest,
    x_full,
    grad_full,
    part,
    box,
    mate,
    rows_out,
    back_part,
    back_box,
    back_mate,
    back_rows_out,
    gate_slope,
    up_slope,
    normed_out,
    hidden_out,
    d_gate_out,
    d_up_out,
    sum_down,
    sum_gate,
    sum_up,
    fresh_down,
    fresh_gate,
    fresh_up,
    pair,
    down,
    rows_given,
    rows_in,
    looked_box,
    x_recv,
    grad_recv,
    box_recv,
    mate_recv,
    back_box_recv,
    back_mate_recv,
    looked_recv,
    part_send,
    rows_send,
    back_part_send,
    back_rows_send,
    x_first,
    grad_first,
    looked_send,
    load_sem,
    store_sem,
    pass_send,
):
    section = lax.axis_index("section")
    me = lax.axis_index("tp")
    batches, own, _ = looked.shape
    chunks, rows, _ = x_full.shape
    owners = rows // own
    groups = peers // owners
    half = peers // 2
    piece = rows // PIECES
    first = section == 0
    final = section == sections - 1
    later = section < sections - 1
    after = section > 0
    left = me < half
    base = jnp.where(left, 0, half)
    depth = jnp.where(left, me, peers - 1 - me)
    middle = depth == half - 1
    inward = jnp.where(left, me + 1, me - 1)
    my_group = me // owners
    my_rows = pl.ds(pl.multiple_of(lax.rem(me, owners) * own, own), own)

    def wait(ref, sem):
        pltpu.make_async_copy(ref, ref, sem).wait()

    def send(source, target, send_sem, recv_sem, device):
        pltpu.make_async_remote_copy(
            src_ref=source,
            dst_ref=target,
            send_sem=send_sem,
            recv_sem=recv_sem,
            device_id=device,
            device_id_type=MESH,
        ).start()

    def around(offset):
        return lax.rem(me + offset, peers)

    loads = (
        pltpu.make_async_copy(pair_here, pair, load_sem.at[0]),
        pltpu.make_async_copy(down_here, down, load_sem.at[1]),
    )
    for load in loads:
        load.start()

    low = section * vocab_part

    def mask(micro):
        inside = (ids[micro] >= low) & (ids[micro] < low + vocab_part)
        rows_given[micro] = jnp.where(inside, looked[micro], jnp.zeros_like(looked[micro]))

    barrier = pltpu.get_barrier_semaphore()
    for offset in range(1, peers):
        pl.semaphore_signal(
            barrier, inc=1, device_id={"tp": around(offset)}, device_id_type=MESH
        )

    @pl.when(later)
    def _():
        for offset in range(peers):
            pl.semaphore_signal(
                barrier,
                inc=1,
                device_id={"section": section + 1, "tp": around(offset)},
                device_id_type=MESH,
            )

    @pl.when(after)
    def _():
        for offset in range(peers):
            pl.semaphore_signal(
                barrier,
                inc=1,
                device_id={"section": section - 1, "tp": around(offset)},
                device_id_type=MESH,
            )

    @pl.when(first)
    def _():
        for other in range(2, sections):
            pl.semaphore_signal(
                barrier, inc=1, device_id={"section": other}, device_id_type=MESH
            )
        pl.semaphore_wait(barrier, 2 * peers - 1 + max(sections - 2, 0))

    @pl.when(section == 1)
    def _():
        pl.semaphore_wait(barrier, (3 if sections > 2 else 2) * peers - 1)

    @pl.when(section >= 2)
    def _():
        pl.semaphore_signal(barrier, inc=1, device_id={"section": 0}, device_id_type=MESH)

    @pl.when((section >= 2) & later)
    def _():
        pl.semaphore_wait(barrier, 3 * peers)

    @pl.when((section >= 2) & final)
    def _():
        pl.semaphore_wait(barrier, 2 * peers)

    def spread(micro, source, full, send_sem, recv_sem, targets):
        chunk = micro * groups + my_group
        for target in targets:
            send(
                source.at[micro],
                full.at[chunk, my_rows],
                send_sem.at[micro],
                recv_sem.at[chunk],
                {"tp": target},
            )
        full[chunk, my_rows, :] = source[micro]

    everyone = [around(offset) for offset in range(1, peers)]
    inside = [base + lax.rem(me - base + offset, half) for offset in range(1, half)]
    across = jnp.where(left, half, half - 1)

    def feed(micro):
        mask(micro)
        total = rows_given[micro]
        for slot in range(sections - 1):
            wait(looked_box.at[slot, micro], looked_recv.at[slot, micro])
            total += looked_box[slot, micro]
        rows_in[micro] = total
        spread(micro, rows_in, x_full, x_first, x_recv, [across] + inside)

    @pl.when(after)
    def _():
        def give(micro, carry):
            mask(micro)
            send(
                rows_given.at[micro],
                looked_box.at[section - 1, micro],
                looked_send.at[micro],
                looked_recv.at[section - 1, micro],
                {"section": 0},
            )
            return carry

        lax.fori_loop(0, batches, give, 0)

    @pl.when(final)
    def _():
        def give(micro, carry):
            spread(micro, seeds, grad_full, grad_first, grad_recv, everyone)
            return carry

        lax.fori_loop(0, batches, give, 0)

    @pl.when(first)
    def _():
        for micro in range(min(FEEDS, batches)):
            feed(micro)

    for total in (sum_down, sum_gate, sum_up):
        total[...] = jnp.zeros_like(total)
    for load in loads:
        load.wait()

    def from_across(chunk):
        return (lax.rem(chunk, groups) < groups // 2) != left

    def pass_on(chunk):
        @pl.when(from_across(chunk))
        def _():
            wait(x_full.at[chunk], x_recv.at[chunk])
            for target in inside:
                send(
                    x_full.at[chunk],
                    x_full.at[chunk],
                    pass_send.at[chunk],
                    x_recv.at[chunk],
                    {"tp": target},
                )

    def arrive(chunk, full, recv_sem, source, passed):
        mine = source & (lax.rem(chunk, groups) == my_group)

        @pl.when(jnp.logical_not(mine | passed))
        def _():
            wait(full.at[chunk], recv_sem.at[chunk])

        if owners > 1:

            @pl.when(mine)
            def _():
                wait(full.at[chunk, pl.ds(0, rows - own)], recv_sem.at[chunk])

    def push(chunk, index, source, box, mate, send_sem, box_sem, mate_sem):
        span = pl.ds(index * piece, piece)

        @pl.when(middle)
        def _():
            send(
                source.at[chunk, span],
                mate.at[chunk, span],
                send_sem.at[chunk],
                mate_sem.at[chunk, index],
                {"tp": peers - 1 - me},
            )

        @pl.when(jnp.logical_not(middle))
        def _():
            send(
                source.at[chunk, span],
                box.at[chunk, span],
                send_sem.at[chunk],
                box_sem.at[chunk, index],
                {"tp": inward},
            )

    def join(chunk, source, box, mate, send_sem, box_sem, mate_sem):
        for index in range(PIECES):
            span = pl.ds(index * piece, piece)
            wait(box.at[chunk, span], box_sem.at[chunk, index])
            total = source[chunk, span, :].astype(jnp.float32)
            total += box[chunk, span, :].astype(jnp.float32)
            source[chunk, span, :] = total.astype(jnp.bfloat16)
            push(chunk, index, source, box, mate, send_sem, box_sem, mate_sem)

    def pass_along(chunk, span, source, full, send_sem, recv_sem, step):
        for offset in range(half):
            send(
                source.at[chunk, span],
                full.at[chunk, span],
                send_sem.at[chunk],
                recv_sem.at[chunk],
                {"section": section + step, "tp": base + offset},
            )

    forward_way = (part, box, mate, part_send, box_recv, mate_recv)
    backward_way = (
        back_part,
        back_box,
        back_mate,
        back_part_send,
        back_box_recv,
        back_mate_recv,
    )

    def forward(chunk):
        arrive(chunk, x_full, x_recv, first, first & middle & from_across(chunk))
        xf = x_full[chunk].astype(jnp.float32)
        normed = (xf * scale_rows(xf)).astype(jnp.bfloat16)
        normed_out[chunk] = normed
        gate = dot_nt(normed, pair[0])
        upper = dot_nt(normed, pair[1])
        sig = jax.nn.sigmoid(gate)
        silu = gate * sig
        hidden = (silu * upper).astype(jnp.bfloat16)
        hidden_out[chunk] = hidden
        gate_slope[chunk] = upper * sig * (1.0 + gate * (1.0 - sig))
        up_slope[chunk] = silu

        @pl.when(later)
        def _():
            part[chunk] = dot(hidden, down[...]).astype(jnp.bfloat16)

            @pl.when(depth == 0)
            def _():
                for index in range(PIECES):
                    push(chunk, index, *forward_way)

    def forward_join(chunk):
        join(chunk, *forward_way)

    def forward_end(chunk):
        for index in range(PIECES):
            span = pl.ds(index * piece, piece)
            wait(mate.at[chunk, span], mate_recv.at[chunk, index])
            total = part[chunk, span, :].astype(jnp.float32)
            total += mate[chunk, span, :].astype(jnp.float32)
            xf = x_full[chunk, span, :].astype(jnp.float32)
            rows_out[chunk, span, :] = (xf + total).astype(jnp.bfloat16)
            pass_along(chunk, span, rows_out, x_full, rows_send, x_recv, 1)

    def backward(chunk):
        arrive(chunk, grad_full, grad_recv, final, section < 0)
        grad = grad_full[chunk]
        d_hidden = dot_nt(grad, down[...])
        d_gate = (d_hidden * gate_slope[chunk]).astype(jnp.bfloat16)
        d_up = (d_hidden * up_slope[chunk]).astype(jnp.bfloat16)
        d_gate_out[chunk] = d_gate
        d_up_out[chunk] = d_up

        @pl.when(after)
        def _():
            back_part[chunk] = (dot(d_gate, pair[0]) + dot(d_up, pair[1])).astype(
                jnp.bfloat16
            )

            @pl.when(depth == 0)
            def _():
                for index in range(PIECES):
                    push(chunk, index, *backward_way)

    def backward_join(chunk):
        join(chunk, *backward_way)

    def backward_end(chunk):
        for index in range(PIECES):
            span = pl.ds(index * piece, piece)
            wait(back_mate.at[chunk, span], back_mate_recv.at[chunk, index])
            d_norm = back_part[chunk, span, :].astype(jnp.float32)
            d_norm += back_mate[chunk, span, :].astype(jnp.float32)
            xf = x_full[chunk, span, :].astype(jnp.float32)
            rinv = scale_rows(xf)
            d_x = (
                grad_full[chunk, span, :].astype(jnp.float32)
                + rinv * d_norm
                - xf * (rinv * rinv * rinv) * jnp.mean(d_norm * xf, axis=-1, keepdims=True)
            )
            back_rows_out[chunk, span, :] = d_x.astype(jnp.bfloat16)
            pass_along(chunk, span, back_rows_out, grad_full, back_rows_send, grad_recv, -1)

    bundle = min(chunks, max(1, WEIGHT_ROWS // rows))
    bundles = chunks // bundle

    top = pl.ds(0, new_gate_top.shape[0])
    rest = pl.ds(new_gate_top.shape[0], new_gate_rest.shape[0])
    stores = (
        (pltpu.make_async_copy(fresh_down, new_down, store_sem.at[0]),),
        (pltpu.make_async_copy(fresh_up, new_up, store_sem.at[1]),),
        (
            pltpu.make_async_copy(fresh_gate.at[top], new_gate_top, store_sem.at[2]),
            pltpu.make_async_copy(fresh_gate.at[rest], new_gate_rest, store_sem.at[3]),
        ),
    )

    def weigh(which, left, right, weights, total, out, copies):
        span = pl.ds(which * bundle, bundle)
        rows_of = bundle * rows
        update = dot_tn(
            left[span].reshape(rows_of, left.shape[2]),
            right[span].reshape(rows_of, right.shape[2]),
        )

        @pl.when(which < bundles - 1)
        def _():
            total[...] += update

        @pl.when(which == bundles - 1)
        def _():
            grads = total[...] + update
            out[...] = (weights.astype(jnp.float32) - INNER_LR * grads).astype(jnp.bfloat16)
            for copy in copies:
                copy.start()

    weighings = (
        lambda which: weigh(
            which, hidden_out, grad_full, down[...], sum_down, fresh_down, stores[0]
        ),
        lambda which: weigh(which, d_up_out, normed_out, pair[1], sum_up, fresh_up, stores[1]),
        lambda which: weigh(
            which, d_gate_out, normed_out, pair[0], sum_gate, fresh_gate, stores[2]
        ),
    )
    ahead = STAGE * section
    behind = STAGE * (2 * (sections - 1) - section)

    def step(tick, carry):
        def on(condition, offset, task):
            chunk = tick - offset

            @pl.when(condition & (chunk >= 0) & (chunk < chunks))
            def _():
                task(chunk)

        fed = tick // groups + FEEDS

        @pl.when(first & (lax.rem(tick, groups) == 0) & (fed < batches))
        def _():
            feed(fed)

        on(first & middle, ahead - PASSES, pass_on)
        on(section >= 0, ahead, forward)
        on(later & (depth > 0), ahead, forward_join)
        on(section >= 0, behind, backward)
        on(after & (depth > 0), behind, backward_join)
        on(later & middle, ahead + 1, forward_end)
        on(after & middle, behind + 1, backward_end)
        for turn, weighing in enumerate(weighings):
            since = tick - behind - (bundle - 1) - turn

            @pl.when((since >= 0) & (since < chunks) & (lax.rem(since, bundle) == 0))
            def _():
                weighing(since // bundle)

        return carry

    @pl.when(first & middle)
    def _():
        for chunk in range(min(PASSES, chunks)):
            pass_on(chunk)

    lax.fori_loop(0, chunks + 2 * STAGE * (sections - 1) + 2, step, 0)

    def drain_feeds(micro, carry):
        others = rows_in.at[pl.ds(0, peers - 1)]

        @pl.when(first)
        def _():
            wait(rows_in.at[pl.ds(0, half)], x_first.at[micro])

        @pl.when(final)
        def _():
            wait(others, grad_first.at[micro])

        @pl.when(after)
        def _():
            wait(rows_given.at[micro], looked_send.at[micro])

        return carry

    lax.fori_loop(0, batches, drain_feeds, 0)

    def drain(chunk, carry):
        if half > 1:

            @pl.when(first & middle & from_across(chunk))
            def _():
                wait(x_full.at[pl.ds(0, half - 1)], pass_send.at[chunk])

        @pl.when(later)
        def _():
            wait(part.at[chunk], part_send.at[chunk])

        @pl.when(after)
        def _():
            wait(back_part.at[chunk], back_part_send.at[chunk])

        @pl.when(later & middle)
        def _():
            wait(rows_out.at[pl.ds(0, half)], rows_send.at[chunk])

        @pl.when(after & middle)
        def _():
            wait(back_rows_out.at[pl.ds(0, half)], back_rows_send.at[chunk])

        return carry

    lax.fori_loop(0, chunks, drain, 0)
    for copies in stores:
        for copy in copies:
            copy.wait()


def run_relay(x0, ids, vocab_part, seeds, pair, down):
    sections, peers = lax.axis_size("section"), lax.axis_size("tp")
    batches, own, width = x0.shape
    hidden = down.shape[0]
    owners = min(OWNERS, peers)
    rows = own * owners
    chunks = batches * peers // owners

    def of(columns, kind=jnp.bfloat16):
        return pltpu.VMEM((chunks, rows, columns), kind)

    def like(kind):
        return pltpu.VMEM((hidden, width), kind)

    def sems(*shape):
        return pltpu.SemaphoreType.DMA(shape)

    vmem = pl.BlockSpec(memory_space=pltpu.VMEM)
    anywhere = pl.BlockSpec(memory_space=pl.ANY)
    cut = hidden // 2
    flops = 2 * chunks * rows * width * hidden * 9
    return pl.pallas_call(
        functools.partial(relay, sections, peers, vocab_part),
        out_shape=tuple(
            pltpu.HBM((size, width), jnp.bfloat16)
            for size in (hidden, hidden, cut, hidden - cut)
        ),
        in_specs=[vmem] * 3 + [anywhere] * 2,
        out_specs=(anywhere,) * 4,
        scratch_shapes=[of(width)] * 10
        + [of(hidden, kind=jnp.float32)] * 2
        + [of(width)]
        + [of(hidden)] * 3
        + [like(jnp.float32)] * 3
        + [like(jnp.bfloat16)] * 3
        + [pltpu.VMEM(pair.shape, jnp.bfloat16), like(jnp.bfloat16)]
        + [pltpu.VMEM((batches, own, width), jnp.bfloat16)]
        + [
            pltpu.VMEM((batches, own, width), jnp.bfloat16),
            pltpu.VMEM((sections - 1, batches, own, width), jnp.bfloat16),
            sems(chunks),
            sems(chunks),
            sems(chunks, PIECES),
            sems(chunks, PIECES),
            sems(chunks, PIECES),
            sems(chunks, PIECES),
            sems(sections - 1, batches),
            sems(chunks),
            sems(chunks),
            sems(chunks),
            sems(chunks),
            sems(batches),
            sems(batches),
            sems(batches),
            sems(2),
            sems(4),
            sems(chunks),
        ],
        compiler_params=pltpu.CompilerParams(
            collective_id=0, has_side_effects=True, vmem_limit_bytes=63 * 1024 * 1024
        ),
        cost_estimate=pl.CostEstimate(
            flops=flops, bytes_accessed=32 * 1024 * 1024, transcendentals=0
        ),
    )(x0, ids, seeds, pair, down)


def outer_step(replicas, *refs):
    shared = [ref[...].astype(jnp.float32) for ref in refs[:replicas]]
    outer, moment = refs[replicas][0], refs[replicas + 1][0]
    new, next_outer, next_moment = refs[-3:]
    mean = outer - sum(shared) / replicas
    moved = MOMENTUM * moment + mean
    stepped = outer - OUTER_LR * (mean + MOMENTUM * moved)
    new[0] = stepped.astype(jnp.bfloat16)
    next_outer[0] = stepped
    next_moment[0] = moved


def keep_step(fresh, outer, moment, *refs):
    new, next_outer, next_moment = refs[-3:]
    new[0] = fresh[...]
    next_outer[...] = outer[...]
    next_moment[...] = moment[...]


def step_part(index, start, shared, outer, moment, earlier):
    replicas = len(shared)
    rows, width = shared[0].shape
    block = next(
        size
        for size in range(min(BLOCK, rows), 0, -1)
        if rows % size == 0 and start % size == 0
    )
    skip = start // block
    one = pl.BlockSpec((block, width), lambda i: (i, 0))
    part = pl.BlockSpec((1, block, width), lambda i: (index, i + skip, 0))
    anywhere = pl.BlockSpec(memory_space=pl.ANY)
    first = replicas + 2

    return pl.pallas_call(
        keep_step if replicas == 1 else functools.partial(outer_step, replicas),
        grid=(rows // block,),
        out_shape=(
            pltpu.HBM(outer.shape, jnp.bfloat16),
            pltpu.HBM(outer.shape, jnp.float32),
            pltpu.HBM(outer.shape, jnp.float32),
        ),
        in_specs=[one] * replicas + [part] * 2 + [anywhere] * len(earlier),
        out_specs=(part,) * 3,
        input_output_aliases={first + place: place for place in range(len(earlier))},
        compiler_params=pltpu.CompilerParams(vmem_limit_bytes=24 * 1024 * 1024),
        cost_estimate=pl.CostEstimate(
            flops=10 * rows * width, bytes_accessed=24 * rows * width, transcendentals=0
        ),
    )(*shared, outer, moment, *earlier)


def shards(
    token_ids,
    embed,
    w_in,
    w_down,
    outer_in,
    outer_down,
    moment_in,
    moment_down,
    cotangent,
    fragment,
):
    section = lax.axis_index("section")
    replicas = lax.axis_size("rep")
    ids = token_ids[0]
    vocab_part, width = embed.shape
    local_ids = ids - section * vocab_part
    looked = jnp.take(embed, local_ids, axis=0, mode="clip")

    def turned(values):
        return jnp.swapaxes(values, -1, -2)

    new_down, new_up, gate_top, gate_rest = run_relay(
        looked, ids[:, :, None], vocab_part, cotangent[0], turned(w_in[0, 0]), w_down[0, 0]
    )

    def shared(values):
        everyone = [values]
        for _ in range(replicas - 1):
            everyone.append(
                lax.ppermute(
                    everyone[-1],
                    "rep",
                    [(source, (source + 1) % replicas) for source in range(replicas)],
                )
            )
        return everyone

    flag = lax.dynamic_index_in_dim(fragment, section, 0, keepdims=False)

    outer_turned, moment_turned = turned(outer_in[0]), turned(moment_in[0])

    def step(gates, more_gates, ups, downs):
        down = step_part(0, 0, downs, outer_down, moment_down, ())
        ins = step_part(1, 0, ups, outer_turned, moment_turned, ())
        ins = step_part(0, 0, gates, outer_turned, moment_turned, ins)
        cut = gates[0].shape[0]
        ins = step_part(0, cut, more_gates, outer_turned, moment_turned, ins)
        return (ins[0], down[0], ins[1], down[1], ins[2], down[2])

    def synchronize():
        return step(shared(gate_top), shared(gate_rest), shared(new_up), shared(new_down))

    def keep():
        return step([gate_top], [gate_rest], [new_up], [new_down])

    new_in, new_down, outer_in, outer_down, moment_in, moment_down = lax.cond(
        flag == 1, synchronize, keep
    )
    return (
        turned(new_in)[None, None],
        new_down[None],
        turned(outer_in)[None],
        outer_down,
        turned(moment_in)[None],
        moment_down,
    )


def solution(mesh):
    return jax.shard_map(
        shards,
        mesh=mesh,
        in_specs=(
            P("rep", None, "tp"),
            P("section", None),
            P("rep", "section", None, None, "tp"),
            P("rep", "section", "tp", None),
            P("section", None, None, "tp"),
            P("section", "tp", None),
            P("section", None, None, "tp"),
            P("section", "tp", None),
            P("rep", None, "tp", None),
            P(),
        ),
        out_specs=(
            P("rep", "section", None, None, "tp"),
            P("rep", "section", "tp", None),
            P("section", None, None, "tp"),
            P("section", "tp", None),
            P("section", None, None, "tp"),
            P("section", "tp", None),
        ),
        check_vma=False,
    )
```

```python
import functools

import jax
import jax.numpy as jnp
from jax import lax
from jax.experimental import pallas as pl
from jax.experimental.pallas import tpu as pltpu
from jax.sharding import PartitionSpec as P

EPS = 1e-05
INNER_LR = 0.001
OUTER_LR = 0.7
MOMENTUM = 0.9
STAGE = 4
OWNERS = 2
PIECES = 2
FEEDS = 4
PASSES = 4
WEIGHT_ROWS = 256
BLOCK = 176
MESH = pl.DeviceIdType.MESH
NT = (((1,), (1,)), ((), ()))
TN = (((0,), (0,)), ((), ()))


def scale_rows(values):
    return lax.rsqrt(jnp.mean(values * values, axis=-1, keepdims=True) + EPS)


def dot(left, right):
    return jnp.dot(left, right, preferred_element_type=jnp.float32)


def dot_nt(left, right):
    return lax.dot_general(left, right, NT, preferred_element_type=jnp.float32)


def dot_tn(left, right):
    return lax.dot_general(left, right, TN, preferred_element_type=jnp.float32)


def relay(
    sections,
    peers,
    vocab_part,
    looked,
    ids,
    seeds,
    pair_here,
    down_here,
    new_down,
    new_up,
    new_gate_top,
    new_gate_rest,
    x_full,
    grad_full,
    part,
    box,
    mate,
    rows_out,
    back_part,
    back_box,
    back_mate,
    back_rows_out,
    gate_slope,
    up_slope,
    normed_out,
    hidden_out,
    d_gate_out,
    d_up_out,
    sum_down,
    sum_gate,
    sum_up,
    fresh_down,
    fresh_gate,
    fresh_up,
    pair,
    down,
    rows_given,
    rows_in,
    looked_box,
    x_recv,
    grad_recv,
    box_recv,
    mate_recv,
    back_box_recv,
    back_mate_recv,
    looked_recv,
    part_send,
    rows_send,
    back_part_send,
    back_rows_send,
    x_first,
    grad_first,
    looked_send,
    load_sem,
    store_sem,
    pass_send,
):
    section = lax.axis_index("section")
    me = lax.axis_index("tp")
    batches, own, _ = looked.shape
    chunks, rows, _ = x_full.shape
    owners = rows // own
    groups = peers // owners
    half = peers // 2
    piece = rows // PIECES
    first = section == 0
    final = section == sections - 1
    later = section < sections - 1
    after = section > 0
    left = me < half
    base = jnp.where(left, 0, half)
    depth = jnp.where(left, me, peers - 1 - me)
    middle = depth == half - 1
    inward = jnp.where(left, me + 1, me - 1)
    my_group = me // owners
    my_rows = pl.ds(pl.multiple_of(lax.rem(me, owners) * own, own), own)

    def wait(ref, sem):
        pltpu.make_async_copy(ref, ref, sem).wait()

    def send(source, target, send_sem, recv_sem, device):
        pltpu.make_async_remote_copy(
            src_ref=source,
            dst_ref=target,
            send_sem=send_sem,
            recv_sem=recv_sem,
            device_id=device,
            device_id_type=MESH,
        ).start()

    def around(offset):
        return lax.rem(me + offset, peers)

    loads = (
        pltpu.make_async_copy(pair_here, pair, load_sem.at[0]),
        pltpu.make_async_copy(down_here, down, load_sem.at[1]),
    )
    for load in loads:
        load.start()

    low = section * vocab_part

    def mask(micro):
        named = ids[pl.ds(micro, 1), :]
        mine = ((named >= low) & (named < low + vocab_part)).astype(jnp.float32)
        across_ids = lax.broadcasted_iota(jnp.int32, (own, own), 0)
        along_ids = lax.broadcasted_iota(jnp.int32, (own, own), 1)
        picked = jnp.where(across_ids == along_ids, jnp.broadcast_to(mine, (own, own)), 0.0)
        inside = jnp.sum(picked, axis=1, keepdims=True) > 0.5
        rows_given[micro] = jnp.where(inside, looked[micro], jnp.zeros_like(looked[micro]))

    barrier = pltpu.get_barrier_semaphore()
    for offset in range(1, peers):
        pl.semaphore_signal(
            barrier, inc=1, device_id={"tp": around(offset)}, device_id_type=MESH
        )

    @pl.when(later)
    def _():
        for offset in range(peers):
            pl.semaphore_signal(
                barrier,
                inc=1,
                device_id={"section": section + 1, "tp": around(offset)},
                device_id_type=MESH,
            )

    @pl.when(after)
    def _():
        for offset in range(peers):
            pl.semaphore_signal(
                barrier,
                inc=1,
                device_id={"section": section - 1, "tp": around(offset)},
                device_id_type=MESH,
            )

    @pl.when(first)
    def _():
        for other in range(2, sections):
            pl.semaphore_signal(
                barrier, inc=1, device_id={"section": other}, device_id_type=MESH
            )
        pl.semaphore_wait(barrier, 2 * peers - 1 + max(sections - 2, 0))

    @pl.when(section == 1)
    def _():
        pl.semaphore_wait(barrier, (3 if sections > 2 else 2) * peers - 1)

    @pl.when(section >= 2)
    def _():
        pl.semaphore_signal(barrier, inc=1, device_id={"section": 0}, device_id_type=MESH)

    @pl.when((section >= 2) & later)
    def _():
        pl.semaphore_wait(barrier, 3 * peers)

    @pl.when((section >= 2) & final)
    def _():
        pl.semaphore_wait(barrier, 2 * peers)

    def spread(micro, source, full, send_sem, recv_sem, targets):
        chunk = micro * groups + my_group
        for target in targets:
            send(
                source.at[micro],
                full.at[chunk, my_rows],
                send_sem.at[micro],
                recv_sem.at[chunk],
                {"tp": target},
            )
        full[chunk, my_rows, :] = source[micro]

    everyone = [around(offset) for offset in range(1, peers)]
    inside = [base + lax.rem(me - base + offset, half) for offset in range(1, half)]
    across = jnp.where(left, half, half - 1)

    def feed(micro):
        mask(micro)
        total = rows_given[micro]
        for slot in range(sections - 1):
            wait(looked_box.at[slot, micro], looked_recv.at[slot, micro])
            total += looked_box[slot, micro]
        rows_in[micro] = total
        spread(micro, rows_in, x_full, x_first, x_recv, [across] + inside)

    @pl.when(after)
    def _():
        def give(micro, carry):
            mask(micro)
            send(
                rows_given.at[micro],
                looked_box.at[section - 1, micro],
                looked_send.at[micro],
                looked_recv.at[section - 1, micro],
                {"section": 0},
            )
            return carry

        lax.fori_loop(0, batches, give, 0)

    @pl.when(final)
    def _():
        def give(micro, carry):
            spread(micro, seeds, grad_full, grad_first, grad_recv, everyone)
            return carry

        lax.fori_loop(0, batches, give, 0)

    @pl.when(first)
    def _():
        for micro in range(min(FEEDS, batches)):
            feed(micro)

    for total in (sum_down, sum_gate, sum_up):
        total[...] = jnp.zeros_like(total)
    for load in loads:
        load.wait()

    def from_across(chunk):
        return (lax.rem(chunk, groups) < groups // 2) != left

    def pass_on(chunk):
        @pl.when(from_across(chunk))
        def _():
            wait(x_full.at[chunk], x_recv.at[chunk])
            for target in inside:
                send(
                    x_full.at[chunk],
                    x_full.at[chunk],
                    pass_send.at[chunk],
                    x_recv.at[chunk],
                    {"tp": target},
                )

    def arrive(chunk, full, recv_sem, source, passed):
        mine = source & (lax.rem(chunk, groups) == my_group)

        @pl.when(jnp.logical_not(mine | passed))
        def _():
            wait(full.at[chunk], recv_sem.at[chunk])

        if owners > 1:

            @pl.when(mine)
            def _():
                wait(full.at[chunk, pl.ds(0, rows - own)], recv_sem.at[chunk])

    def push(chunk, index, source, box, mate, send_sem, box_sem, mate_sem):
        span = pl.ds(index * piece, piece)

        @pl.when(middle)
        def _():
            send(
                source.at[chunk, span],
                mate.at[chunk, span],
                send_sem.at[chunk],
                mate_sem.at[chunk, index],
                {"tp": peers - 1 - me},
            )

        @pl.when(jnp.logical_not(middle))
        def _():
            send(
                source.at[chunk, span],
                box.at[chunk, span],
                send_sem.at[chunk],
                box_sem.at[chunk, index],
                {"tp": inward},
            )

    def join(chunk, source, box, mate, send_sem, box_sem, mate_sem):
        for index in range(PIECES):
            span = pl.ds(index * piece, piece)
            wait(box.at[chunk, span], box_sem.at[chunk, index])
            total = source[chunk, span, :].astype(jnp.float32)
            total += box[chunk, span, :].astype(jnp.float32)
            source[chunk, span, :] = total.astype(jnp.bfloat16)
            push(chunk, index, source, box, mate, send_sem, box_sem, mate_sem)

    def pass_along(chunk, span, source, full, send_sem, recv_sem, step):
        for offset in range(half):
            send(
                source.at[chunk, span],
                full.at[chunk, span],
                send_sem.at[chunk],
                recv_sem.at[chunk],
                {"section": section + step, "tp": base + offset},
            )

    forward_way = (part, box, mate, part_send, box_recv, mate_recv)
    backward_way = (
        back_part,
        back_box,
        back_mate,
        back_part_send,
        back_box_recv,
        back_mate_recv,
    )

    def forward(chunk):
        arrive(chunk, x_full, x_recv, first, first & middle & from_across(chunk))
        xf = x_full[chunk].astype(jnp.float32)
        normed = (xf * scale_rows(xf)).astype(jnp.bfloat16)
        normed_out[chunk] = normed
        gate = dot_nt(normed, pair[0])
        upper = dot_nt(normed, pair[1])
        sig = jax.nn.sigmoid(gate)
        silu = gate * sig
        hidden = (silu * upper).astype(jnp.bfloat16)
        hidden_out[chunk] = hidden
        gate_slope[chunk] = upper * sig * (1.0 + gate * (1.0 - sig))
        up_slope[chunk] = silu

        @pl.when(later)
        def _():
            part[chunk] = dot(hidden, down[...]).astype(jnp.bfloat16)

            @pl.when(depth == 0)
            def _():
                for index in range(PIECES):
                    push(chunk, index, *forward_way)

    def forward_join(chunk):
        join(chunk, *forward_way)

    def forward_end(chunk):
        for index in range(PIECES):
            span = pl.ds(index * piece, piece)
            wait(mate.at[chunk, span], mate_recv.at[chunk, index])
            total = part[chunk, span, :].astype(jnp.float32)
            total += mate[chunk, span, :].astype(jnp.float32)
            xf = x_full[chunk, span, :].astype(jnp.float32)
            rows_out[chunk, span, :] = (xf + total).astype(jnp.bfloat16)
            pass_along(chunk, span, rows_out, x_full, rows_send, x_recv, 1)

    def backward(chunk):
        arrive(chunk, grad_full, grad_recv, final, section < 0)
        grad = grad_full[chunk]
        d_hidden = dot_nt(grad, down[...])
        d_gate = (d_hidden * gate_slope[chunk]).astype(jnp.bfloat16)
        d_up = (d_hidden * up_slope[chunk]).astype(jnp.bfloat16)
        d_gate_out[chunk] = d_gate
        d_up_out[chunk] = d_up

        @pl.when(after)
        def _():
            back_part[chunk] = (dot(d_gate, pair[0]) + dot(d_up, pair[1])).astype(
                jnp.bfloat16
            )

            @pl.when(depth == 0)
            def _():
                for index in range(PIECES):
                    push(chunk, index, *backward_way)

    def backward_join(chunk):
        join(chunk, *backward_way)

    def backward_end(chunk):
        for index in range(PIECES):
            span = pl.ds(index * piece, piece)
            wait(back_mate.at[chunk, span], back_mate_recv.at[chunk, index])
            d_norm = back_part[chunk, span, :].astype(jnp.float32)
            d_norm += back_mate[chunk, span, :].astype(jnp.float32)
            xf = x_full[chunk, span, :].astype(jnp.float32)
            rinv = scale_rows(xf)
            d_x = (
                grad_full[chunk, span, :].astype(jnp.float32)
                + rinv * d_norm
                - xf * (rinv * rinv * rinv) * jnp.mean(d_norm * xf, axis=-1, keepdims=True)
            )
            back_rows_out[chunk, span, :] = d_x.astype(jnp.bfloat16)
            pass_along(chunk, span, back_rows_out, grad_full, back_rows_send, grad_recv, -1)

    bundle = min(chunks, max(1, WEIGHT_ROWS // rows))
    bundles = chunks // bundle

    top = pl.ds(0, new_gate_top.shape[0])
    rest = pl.ds(new_gate_top.shape[0], new_gate_rest.shape[0])
    stores = (
        (pltpu.make_async_copy(fresh_down, new_down, store_sem.at[0]),),
        (pltpu.make_async_copy(fresh_up, new_up, store_sem.at[1]),),
        (
            pltpu.make_async_copy(fresh_gate.at[top], new_gate_top, store_sem.at[2]),
            pltpu.make_async_copy(fresh_gate.at[rest], new_gate_rest, store_sem.at[3]),
        ),
    )

    def weigh(which, left, right, weights, total, out, copies):
        span = pl.ds(which * bundle, bundle)
        rows_of = bundle * rows
        update = dot_tn(
            left[span].reshape(rows_of, left.shape[2]),
            right[span].reshape(rows_of, right.shape[2]),
        )

        @pl.when(which < bundles - 1)
        def _():
            total[...] += update

        @pl.when(which == bundles - 1)
        def _():
            grads = total[...] + update
            out[...] = (weights.astype(jnp.float32) - INNER_LR * grads).astype(jnp.bfloat16)
            for copy in copies:
                copy.start()

    weighings = (
        lambda which: weigh(
            which, hidden_out, grad_full, down[...], sum_down, fresh_down, stores[0]
        ),
        lambda which: weigh(which, d_up_out, normed_out, pair[1], sum_up, fresh_up, stores[1]),
        lambda which: weigh(
            which, d_gate_out, normed_out, pair[0], sum_gate, fresh_gate, stores[2]
        ),
    )
    ahead = STAGE * section
    behind = STAGE * (2 * (sections - 1) - section)

    def step(tick, carry):
        def on(condition, offset, task):
            chunk = tick - offset

            @pl.when(condition & (chunk >= 0) & (chunk < chunks))
            def _():
                task(chunk)

        fed = tick // groups + FEEDS

        @pl.when(first & (lax.rem(tick, groups) == 0) & (fed < batches))
        def _():
            feed(fed)

        on(first & middle, ahead - PASSES, pass_on)
        on(section >= 0, ahead, forward)
        on(later & (depth > 0), ahead, forward_join)
        on(section >= 0, behind, backward)
        on(after & (depth > 0), behind, backward_join)
        on(later & middle, ahead + 1, forward_end)
        on(after & middle, behind + 1, backward_end)
        for turn, weighing in enumerate(weighings):
            since = tick - behind - (bundle - 1) - turn

            @pl.when((since >= 0) & (since < chunks) & (lax.rem(since, bundle) == 0))
            def _():
                weighing(since // bundle)

        return carry

    @pl.when(first & middle)
    def _():
        for chunk in range(min(PASSES, chunks)):
            pass_on(chunk)

    lax.fori_loop(0, chunks + 2 * STAGE * (sections - 1) + 2, step, 0)

    def drain_feeds(micro, carry):
        others = rows_in.at[pl.ds(0, peers - 1)]

        @pl.when(first)
        def _():
            wait(rows_in.at[pl.ds(0, half)], x_first.at[micro])

        @pl.when(final)
        def _():
            wait(others, grad_first.at[micro])

        @pl.when(after)
        def _():
            wait(rows_given.at[micro], looked_send.at[micro])

        return carry

    lax.fori_loop(0, batches, drain_feeds, 0)

    def drain(chunk, carry):
        if half > 1:

            @pl.when(first & middle & from_across(chunk))
            def _():
                wait(x_full.at[pl.ds(0, half - 1)], pass_send.at[chunk])

        @pl.when(later)
        def _():
            wait(part.at[chunk], part_send.at[chunk])

        @pl.when(after)
        def _():
            wait(back_part.at[chunk], back_part_send.at[chunk])

        @pl.when(later & middle)
        def _():
            wait(rows_out.at[pl.ds(0, half)], rows_send.at[chunk])

        @pl.when(after & middle)
        def _():
            wait(back_rows_out.at[pl.ds(0, half)], back_rows_send.at[chunk])

        return carry

    lax.fori_loop(0, chunks, drain, 0)
    for copies in stores:
        for copy in copies:
            copy.wait()


def run_relay(x0, ids, vocab_part, seeds, pair, down):
    sections, peers = lax.axis_size("section"), lax.axis_size("tp")
    batches, own, width = x0.shape
    hidden = down.shape[0]
    owners = min(OWNERS, peers)
    rows = own * owners
    chunks = batches * peers // owners

    def of(columns, kind=jnp.bfloat16):
        return pltpu.VMEM((chunks, rows, columns), kind)

    def like(kind):
        return pltpu.VMEM((hidden, width), kind)

    def sems(*shape):
        return pltpu.SemaphoreType.DMA(shape)

    vmem = pl.BlockSpec(memory_space=pltpu.VMEM)
    anywhere = pl.BlockSpec(memory_space=pl.ANY)
    cut = hidden // 2
    flops = 2 * chunks * rows * width * hidden * 9
    return pl.pallas_call(
        functools.partial(relay, sections, peers, vocab_part),
        out_shape=tuple(
            pltpu.HBM((size, width), jnp.bfloat16)
            for size in (hidden, hidden, cut, hidden - cut)
        ),
        in_specs=[vmem] * 3 + [anywhere] * 2,
        out_specs=(anywhere,) * 4,
        scratch_shapes=[of(width)] * 10
        + [of(hidden, kind=jnp.float32)] * 2
        + [of(width)]
        + [of(hidden)] * 3
        + [like(jnp.float32)] * 3
        + [like(jnp.bfloat16)] * 3
        + [pltpu.VMEM(pair.shape, jnp.bfloat16), like(jnp.bfloat16)]
        + [pltpu.VMEM((batches, own, width), jnp.bfloat16)]
        + [
            pltpu.VMEM((batches, own, width), jnp.bfloat16),
            pltpu.VMEM((sections - 1, batches, own, width), jnp.bfloat16),
            sems(chunks),
            sems(chunks),
            sems(chunks, PIECES),
            sems(chunks, PIECES),
            sems(chunks, PIECES),
            sems(chunks, PIECES),
            sems(sections - 1, batches),
            sems(chunks),
            sems(chunks),
            sems(chunks),
            sems(chunks),
            sems(batches),
            sems(batches),
            sems(batches),
            sems(2),
            sems(4),
            sems(chunks),
        ],
        compiler_params=pltpu.CompilerParams(
            collective_id=0, has_side_effects=True, vmem_limit_bytes=63 * 1024 * 1024
        ),
        cost_estimate=pl.CostEstimate(
            flops=flops, bytes_accessed=32 * 1024 * 1024, transcendentals=0
        ),
    )(x0, ids, seeds, pair, down)


def outer_step(replicas, *refs):
    shared = [ref[...].astype(jnp.float32) for ref in refs[:replicas]]
    outer, moment = refs[replicas][0], refs[replicas + 1][0]
    new, next_outer, next_moment = refs[-3:]
    mean = outer - sum(shared) / replicas
    moved = MOMENTUM * moment + mean
    stepped = outer - OUTER_LR * (mean + MOMENTUM * moved)
    new[0] = stepped.astype(jnp.bfloat16)
    next_outer[0] = stepped
    next_moment[0] = moved


def keep_step(fresh, outer, moment, *refs):
    new, next_outer, next_moment = refs[-3:]
    new[0] = fresh[...]
    next_outer[...] = outer[...]
    next_moment[...] = moment[...]


def step_part(index, start, shared, outer, moment, earlier, after=()):
    replicas = len(shared)
    rows, width = shared[0].shape
    block = next(
        size
        for size in range(min(BLOCK, rows), 0, -1)
        if rows % size == 0 and start % size == 0
    )
    skip = start // block
    one = pl.BlockSpec((block, width), lambda i: (i, 0))
    part = pl.BlockSpec((1, block, width), lambda i: (index, i + skip, 0))
    anywhere = pl.BlockSpec(memory_space=pl.ANY)
    first = replicas + 2

    return pl.pallas_call(
        keep_step if replicas == 1 else functools.partial(outer_step, replicas),
        grid=(rows // block,),
        out_shape=(
            pltpu.HBM(outer.shape, jnp.bfloat16),
            pltpu.HBM(outer.shape, jnp.float32),
            pltpu.HBM(outer.shape, jnp.float32),
        ),
        in_specs=[one] * replicas + [part] * 2 + [anywhere] * len(earlier + after),
        out_specs=(part,) * 3,
        input_output_aliases={first + place: place for place in range(len(earlier))},
        compiler_params=pltpu.CompilerParams(vmem_limit_bytes=24 * 1024 * 1024),
        cost_estimate=pl.CostEstimate(
            flops=10 * rows * width, bytes_accessed=24 * rows * width, transcendentals=0
        ),
    )(*shared, outer, moment, *earlier, *after)


def shards(
    token_ids,
    embed,
    w_in,
    w_down,
    outer_in,
    outer_down,
    moment_in,
    moment_down,
    cotangent,
    fragment,
):
    section = lax.axis_index("section")
    replicas = lax.axis_size("rep")
    ids = token_ids[0]
    vocab_part, width = embed.shape
    local_ids = ids - section * vocab_part
    looked = jnp.take(embed, local_ids, axis=0, mode="clip")

    def turned(values):
        return jnp.swapaxes(values, -1, -2)

    new_down, new_up, gate_top, gate_rest = run_relay(
        looked, ids, vocab_part, cotangent[0], turned(w_in[0, 0]), w_down[0, 0]
    )

    def shared(values):
        everyone = [values]
        for _ in range(replicas - 1):
            everyone.append(
                lax.ppermute(
                    everyone[-1],
                    "rep",
                    [(source, (source + 1) % replicas) for source in range(replicas)],
                )
            )
        return everyone

    flag = lax.dynamic_index_in_dim(fragment, section, 0, keepdims=False)

    outer_turned, moment_turned = turned(outer_in[0]), turned(moment_in[0])

    def step(gates, more_gates, ups, downs):
        ins = step_part(1, 0, ups, outer_turned, moment_turned, ())
        down = step_part(0, 0, downs, outer_down, moment_down, (), ins[:1])
        ins = step_part(0, 0, gates, outer_turned, moment_turned, ins, down[:1])
        cut = gates[0].shape[0]
        ins = step_part(0, cut, more_gates, outer_turned, moment_turned, ins)
        return (ins[0], down[0], ins[1], down[1], ins[2], down[2])

    def synchronize():
        return step(shared(gate_top), shared(gate_rest), shared(new_up), shared(new_down))

    def keep():
        return step([gate_top], [gate_rest], [new_up], [new_down])

    new_in, new_down, outer_in, outer_down, moment_in, moment_down = lax.cond(
        flag == 1, synchronize, keep
    )
    return (
        turned(new_in)[None, None],
        new_down[None],
        turned(outer_in)[None],
        outer_down,
        turned(moment_in)[None],
        moment_down,
    )


def solution(mesh):
    return jax.shard_map(
        shards,
        mesh=mesh,
        in_specs=(
            P("rep", None, "tp"),
            P("section", None),
            P("rep", "section", None, None, "tp"),
            P("rep", "section", "tp", None),
            P("section", None, None, "tp"),
            P("section", "tp", None),
            P("section", None, None, "tp"),
            P("section", "tp", None),
            P("rep", None, "tp", None),
            P(),
        ),
        out_specs=(
            P("rep", "section", None, None, "tp"),
            P("rep", "section", "tp", None),
            P("section", None, None, "tp"),
            P("section", "tp", None),
            P("section", None, None, "tp"),
            P("section", "tp", None),
        ),
        check_vma=False,
    )
```
